32 devices in a mesh: dp: 8 (over z, x), expert: 4 (over y, core).
Axes of the slice: x: 2, y: 2, z: 4, core: 2. Of those that a mesh axis runs over, the one named last changes fastest.
Arguments:
- tokens: bfloat16 [2048, 2048], P('dp'), may hold values from -6 to 6
- routes: int32 [2048, 6], P('dp'), may hold values from 0 to 63, all different within a row; in each aligned block of 256 rows (0 to 255, 256 to 511, ...) at most 32 rows name the same one
- gates: float32 [2048, 6], P('dp'), may hold values from 0.1 to 1
- w_gate: bfloat16 [64, 2048, 1408], P('dp', None, 'expert'), may hold values from -0.125 to 0.125
- w_up: bfloat16 [64, 2048, 1408], P('dp', None, 'expert'), may hold values from -0.125 to 0.125
- w_down: bfloat16 [64, 1408, 2048], P('dp', 'expert'), may hold values from -0.21875 to 0.21875
- s_gate: bfloat16 [2048, 2816], P(None, 'expert'), may hold values from -0.125 to 0.125
- s_up: bfloat16 [2048, 2816], P(None, 'expert'), may hold values from -0.125 to 0.125
- s_down: bfloat16 [2816, 2048], P('expert'), may hold values from -0.15625 to 0.15625
Outputs:
- mixed: bfloat16 [2048, 2048], P('dp', 'expert')
The draws below stay inside these ranges and needn't reach their ends.
Inputs may be any that keep to these rules, and one draw needn't show every extreme that they name: `routes`: each row names 6 different experts. Within each aligned block of 256 rows (the rows of one index of dp) no expert is named by more than 32 rows; some expert is named by exactly 32 rows in some block of every draw.
All inputs are finite; a program needn't handle non-finite values.
Results may differ from the reference program's by a relative error of at most 0.013.
Values may be sent and summed in bfloat16 or wider, within the bound.
A program may use at most 128 MiB of HBM per device.

```python
import math
import jax
import jax.numpy as jnp
import numpy as np
from jax import lax

D = 2048
FF = 1408
SFF = 2816
EXPERTS = 64
TOP = 6
TOK_DEV = 256
CAP = 32
TOKENS = 2048
N_DP = 8
N_EXPERT = 4


def strengthened(values, own_key, source, target, shards_of, factor):
    def block_of(axis_at):
        return (jnp.arange(values.shape[axis_at]) // (values.shape[axis_at] // shards_of)).reshape((-1,) + (1,) * (values.ndim - 1 - axis_at))

    near = jax.random.permutation(own_key, shards_of)[block_of(target)]
    second = (block_of(target) + shards_of // 2) % shards_of
    return jnp.where((block_of(source) == near) | (block_of(source) == second), factor * values, values)


def level_of(rng, extent, shards, least, largest):
    def one(axis_at, blocks):
        steps = jax.random.uniform(jax.random.fold_in(jax.random.fold_in(rng, 6), axis_at), (blocks,), jnp.float32, least / len(shards), largest / len(shards))
        return jnp.repeat(jnp.exp(steps), extent[axis_at] // blocks).reshape((-1,) + (1,) * (len(extent) - axis_at - 1))

    gain = one(*shards[0])
    for cut in shards[1:]:
        gain = gain * one(*cut)
    return gain


def assign_block(rng, own, number, rows, amount, top, reach, lean):
    ranking = jax.random.permutation(rng, amount)
    heavy_load, common = shares(amount, rows * top, reach, lean, True), shares(amount, rows * top, reach, lean, False)
    places = jnp.arange(amount)

    def named(sizes, turn):
        used = int((sizes > 0).sum())
        fixed = max(1, used // 4)
        moved = fixed + (places - fixed + turn * (used - fixed)) % max(1, amount - fixed)
        return jnp.zeros((amount,), jnp.int32).at[ranking[jnp.where(places < fixed, places, moved)]].set(jnp.asarray(sizes, jnp.int32))

    sizes = jnp.where(number % 4 == 0, named(heavy_load, number // 4), named(common, number - number // 4 - 1))
    mixed = jax.random.permutation(jax.random.fold_in(own, 3), amount)
    donor, taker = mixed[0:amount // 2 * 2:2], mixed[1:amount // 2 * 2:2]
    room = jnp.minimum(sizes[donor] - 1, reach - sizes[taker]) // 2
    room = jnp.where((donor == ranking[0]) | (taker == ranking[0]) | (sizes[taker] == 0), 0, jnp.maximum(room, 0))
    moved = jax.random.randint(jax.random.fold_in(own, 4), (amount // 2,), 0, 1 << 20) % (room + 1)
    sizes = sizes.at[donor].add(-moved).at[taker].add(moved)
    members = jnp.searchsorted(jnp.cumsum(sizes), jnp.arange(rows * top), side="right").astype(jnp.int32)
    grid = members.reshape(top, rows).T
    grid = grid[jax.random.permutation(jax.random.fold_in(own, 1), rows)]
    turn = jax.random.randint(jax.random.fold_in(own, 2), (rows, 1), 0, top)
    return jnp.take_along_axis(grid, (jnp.arange(top)[None, :] + turn) % top, axis=1)


def shares(amount, total, most, skew, full):
    weights = [(1 << 20) // math.isqrt(standing ** skew) + 1 for standing in range(1, amount + 1)]
    largest = most if full else min(most, max(-(-total // amount), total * weights[0] // sum(weights)))
    least = 1 if total - largest >= amount - 1 else 0
    given, spare = [largest] + [least] * (amount - 1), total - largest - least * (amount - 1)
    while spare > 0:
        candidates = [i for i in range(1, amount) if given[i] < largest] or [i for i in range(1, amount) if given[i] < most]
        mass, left = sum([weights[i] for i in candidates]), spare
        for i in candidates:
            more = min(most - given[i], max(1, left * weights[i] // mass), spare)
            given[i] = given[i] + more
            spare = spare - more
    return np.array(given)


def noise(rng, extent, deviation, reach, split=(), kind=jnp.bfloat16):
    gain = level_of(rng, extent, split, -0.22, 0.18) if split else 1.0
    array = jax.random.normal(rng, extent, jnp.float32) * deviation * gain
    return jnp.minimum(jnp.maximum(array, -reach), reach).astype(kind)


def bell_draw_with(own_key, dims, spread, bound, split, heavy, kind=jnp.bfloat16):
    result = spread * jax.random.normal(own_key, dims, jnp.float32)
    if split:
        result = result * level_of(own_key, dims, split, -0.22, 0.18)
    return jnp.clip(strengthened(result, jax.random.fold_in(own_key, 3), *heavy), -bound, bound).astype(kind)


def setup_inputs(seed: int = 0) -> dict:
    splits = jax.random.split(jax.random.key(seed), 10)
    tokens = noise(splits[0], (TOKENS, D), 1.0, 6.0, ((0, 8),))
    routes_keys = jax.random.split(jax.random.fold_in(splits[1], 1), TOKENS // TOK_DEV)
    routes_turns = jax.random.permutation(jax.random.fold_in(splits[1], 3), TOKENS // TOK_DEV)
    routes = jax.vmap(lambda own, number: assign_block(jax.random.fold_in(splits[1], 2), own, number, TOK_DEV, EXPERTS, TOP, CAP, 2))(routes_keys, routes_turns).reshape((TOKENS, TOP))
    gates = jnp.clip(jnp.exp(math.log(1.0) - 2.3025851 * jax.random.uniform(splits[2], (TOKENS, TOP), jnp.float32) ** level_of(splits[2], (TOKENS, TOP), ((0, 8),), -0.2, 0.2)), 0.1, 1.0)
    w_gate = noise(splits[3], (EXPERTS, D, FF), D ** -0.5, 0.125, ((0, 8), (2, 4)))
    w_up = noise(splits[4], (EXPERTS, D, FF), D ** -0.5, 0.125, ((0, 8), (2, 4)))
    w_down = bell_draw_with(splits[5], (EXPERTS, FF, D), FF ** -0.5, 0.21875, ((0, 8), (1, 4)), (1, 2, 4, 2.0))
    s_gate = noise(splits[6], (D, SFF), D ** -0.5, 0.125, ((1, 4),))
    s_up = noise(splits[7], (D, SFF), D ** -0.5, 0.125, ((1, 4),))
    s_down = bell_draw_with(splits[8], (SFF, D), SFF ** -0.5, 0.15625, ((0, 4),), (0, 1, 4, 2.0))
    return {"tokens": tokens, "routes": routes, "gates": gates, "w_gate": w_gate, "w_up": w_up, "w_down": w_down, "s_gate": s_gate, "s_up": s_up, "s_down": s_down}


def quarter_sum(hidden, down, parts):
    inner = hidden.shape[1] // parts
    partial_value = jnp.einsum("rqf,qfd->rqd", hidden.reshape(hidden.shape[0], parts, inner).astype(jnp.float32), down.reshape(parts, inner, down.shape[1]).astype(jnp.float32))
    rounded = lax.optimization_barrier(partial_value.astype(jnp.bfloat16))
    return jnp.sum(rounded.astype(jnp.float32), axis=1)


def reference(tokens, routes, gates, w_gate, w_up, w_down, s_gate, s_up, s_down):
    blocks = routes.reshape(N_DP, TOK_DEV, TOP)
    labels = jnp.arange(EXPERTS, dtype=jnp.int32)
    matches = (blocks[:, :, :, None] == labels[None, None, None, :]).astype(jnp.int32)
    counts = jnp.sum(matches, axis=2).astype(jnp.int32)
    before = (jnp.cumsum(counts, axis=1) - counts).astype(jnp.int32)
    slots = jnp.sum(matches * before[:, :, None, :], axis=3).astype(jnp.int32)
    owner_block = jnp.arange(N_DP, dtype=jnp.int32)[:, None, None]
    dest = ((blocks * N_DP + owner_block) * CAP + slots).astype(jnp.int32)
    token_ids = owner_block * TOK_DEV + jnp.arange(TOK_DEV, dtype=jnp.int32)[None, :, None] + jnp.zeros((1, 1, TOP), jnp.int32)
    sources = jnp.full((EXPERTS * N_DP * CAP,), TOKENS, jnp.int32).at[dest.reshape(-1)].set(token_ids.reshape(-1).astype(jnp.int32))
    padded = jnp.concatenate([tokens, jnp.zeros((1, D), tokens.dtype)], axis=0)

    def one_expert(inputs):
        table, gate_w, up_w, down_w = inputs
        rows = padded[table]
        gate = jnp.dot(rows, gate_w, preferred_element_type=jnp.float32)
        up = jnp.dot(rows, up_w, preferred_element_type=jnp.float32)
        hidden = (jax.nn.silu(gate) * up).astype(jnp.bfloat16)
        return quarter_sum(hidden, down_w, N_EXPERT).astype(jnp.bfloat16)

    outputs = lax.map(one_expert, (sources.reshape(EXPERTS, N_DP * CAP), w_gate, w_up, w_down))
    flat = outputs.reshape(EXPERTS * N_DP * CAP, D)
    picked = flat[dest.reshape(TOKENS, TOP)].astype(jnp.float32)
    routed = jnp.einsum("tk,tkd->td", gates.astype(jnp.float32), picked)
    shared_gate = jnp.dot(tokens, s_gate, preferred_element_type=jnp.float32)
    shared_up = jnp.dot(tokens, s_up, preferred_element_type=jnp.float32)
    shared_hidden = (jax.nn.silu(shared_gate) * shared_up).astype(jnp.bfloat16)
    shared_out = quarter_sum(shared_hidden, s_down, N_EXPERT)
    return (shared_out + routed).astype(jnp.bfloat16)
```

```python
import jax
import jax.numpy as jnp
from jax import lax
from jax.experimental import pallas as pl
from jax.experimental.pallas import tpu as pltpu
from jax.sharding import PartitionSpec as P

CAP = 32
EXTRA = 128
AXES = ("dp", "expert")


def experts_kernel(x_ref, g_ref, wg_ref, wu_ref, wd_ref, out_ref):
    groups, cap, width = x_ref.shape
    members, _, _, part = out_ref.shape
    x = x_ref[...].reshape(groups * cap, width)
    gate = jnp.dot(x, wg_ref[0], preferred_element_type=jnp.float32)
    up = jnp.dot(x, wu_ref[0], preferred_element_type=jnp.float32)
    scale = g_ref[0]
    hidden = (gate / (1.0 + jnp.exp(-gate)) * up * scale).astype(jnp.bfloat16)
    for f in range(members):
        value = jnp.dot(
            hidden, wd_ref[0, :, f * part:(f + 1) * part], preferred_element_type=jnp.float32
        )
        out_ref[f] = value.astype(jnp.bfloat16).reshape(groups, cap, part)


def run_experts(x, slot_gates, w_gate, w_up, w_down, members):
    groups, slots, width = x.shape
    local, _, units = w_gate.shape
    cap = slots // local
    rows = groups * cap
    part = width // members
    return pl.pallas_call(
        experts_kernel,
        grid=(local,),
        out_shape=jax.ShapeDtypeStruct((members, groups, slots, part), jnp.bfloat16),
        in_specs=[
            pl.BlockSpec((groups, cap, width), lambda e: (0, e, 0)),
            pl.BlockSpec((1, rows, 1), lambda e: (e, 0, 0)),
            pl.BlockSpec((1, width, units), lambda e: (e, 0, 0)),
            pl.BlockSpec((1, width, units), lambda e: (e, 0, 0)),
            pl.BlockSpec((1, units, width), lambda e: (e, 0, 0)),
        ],
        out_specs=pl.BlockSpec((members, groups, cap, part), lambda e: (0, 0, e, 0)),
        compiler_params=pltpu.CompilerParams(
            dimension_semantics=("arbitrary",), vmem_limit_bytes=60 << 20
        ),
        cost_estimate=pl.CostEstimate(
            flops=6 * rows * local * width * units,
            bytes_accessed=6 * local * width * units + 4 * rows * local * width,
            transcendentals=rows * local * units,
        ),
    )(x, slot_gates, w_gate, w_up, w_down)


def body(tokens, routes, gates, w_gate, w_up, w_down, s_gate, s_up, s_down):
    tok_rows, width = tokens.shape
    local = w_gate.shape[0]
    groups = lax.axis_size("dp")
    members = lax.axis_size("expert")
    top = routes.shape[1]
    part = width // members
    mine = tok_rows // members
    group = lax.axis_index("dp")
    member = lax.axis_index("expert")

    high = lax.reduce_precision(gates, 8, 7)
    middle = lax.reduce_precision(gates - high, 8, 7)
    low = gates - high - middle
    extra = jnp.concatenate([routes.astype(jnp.float32), high, middle, low], axis=1)
    extra = jnp.pad(extra.astype(jnp.bfloat16), ((0, 0), (0, EXTRA - extra.shape[1])))
    block = jnp.concatenate([tokens, extra], axis=1)
    block = lax.dynamic_slice_in_dim(block, member * mine, mine, 0)
    gathered = lax.all_gather(block, AXES, axis=0, tiled=True)

    shared_gate = jnp.dot(tokens, s_gate, preferred_element_type=jnp.float32)
    shared_up = jnp.dot(tokens, s_up, preferred_element_type=jnp.float32)
    shared_hidden = (jax.nn.silu(shared_gate) * shared_up).astype(jnp.bfloat16)
    shared_part = jnp.dot(shared_hidden, s_down, preferred_element_type=jnp.float32)

    gathered = gathered.reshape(groups, tok_rows, width + EXTRA)
    table = gathered[:, :, width:width + 4 * top].astype(jnp.float32)
    names = table[:, :, :top]
    values = table[:, :, top:2 * top] + table[:, :, 2 * top:3 * top] + table[:, :, 3 * top:]
    own = (group * local + jnp.arange(local)).astype(jnp.float32)
    hits = names[:, :, :, None] == own
    match = jnp.any(hits, axis=2)
    weight = jnp.sum(jnp.where(hits, values[:, :, :, None], 0.0), axis=2)
    earlier = jnp.tri(tok_rows, tok_rows, -1, dtype=jnp.bfloat16)
    before = jnp.einsum(
        "tu,suj->sjt", earlier, match.astype(jnp.bfloat16), preferred_element_type=jnp.float32
    )
    before = jnp.where(jnp.swapaxes(match, 1, 2), before, -1.0)
    slot = jnp.arange(CAP).astype(jnp.float32)
    chosen = before[:, :, None, :] == slot[:, None]
    slot_gates = jnp.sum(
        jnp.where(chosen, jnp.swapaxes(weight, 1, 2)[:, :, None, :], 0.0), axis=3
    )
    slot_gates = jnp.swapaxes(slot_gates, 0, 1).reshape(local, groups * CAP, 1)
    pick = chosen.astype(jnp.bfloat16).reshape(groups, local * CAP, tok_rows)

    x = jnp.einsum(
        "sqt,std->sqd", pick, gathered[:, :, :width], preferred_element_type=jnp.float32
    ).astype(jnp.bfloat16)
    outs = run_experts(x, slot_gates, w_gate, w_up, w_down, members)
    total = jnp.einsum("sqt,fsqd->sftd", pick, outs, preferred_element_type=jnp.float32)
    here = (jnp.arange(groups) == group)[:, None, None, None]
    shared = jnp.swapaxes(shared_part.reshape(tok_rows, members, part), 0, 1)
    total = (total + jnp.where(here, shared[None], 0.0)).astype(jnp.bfloat16)
    total = total.reshape(groups * members, tok_rows, part)
    return lax.psum_scatter(total, AXES, scatter_dimension=0, tiled=False)


def solution(mesh):
    placed = (
        P("dp", None),
        P("dp", None),
        P("dp", None),
        P("dp", None, "expert"),
        P("dp", None, "expert"),
        P("dp", "expert", None),
        P(None, "expert"),
        P(None, "expert"),
        P("expert", None),
    )
    return jax.shard_map(
        body, mesh=mesh, in_specs=placed, out_specs=P("dp", "expert"), check_vma=False
    )
```
